32 devices in a mesh: occ: 4 (over y, core), vir: 8 (over z, x).
Axes of the slice: x: 2, y: 2, z: 4, core: 2. Of those that a mesh axis runs over, the one named last changes fastest.
Arguments:
- amplitudes: bfloat16 [2048, 4096], P('occ', 'vir'), may hold values from -6 to 6
- hole_integrals: bfloat16 [2048, 2048], P('occ'), may hold values from -0.375 to 0.375
- particle_integrals: bfloat16 [4096, 4096], P('vir'), may hold values from -0.375 to 0.375
- occ_irrep: int32 [32], replicated, may hold values from 0 to 7
- vir_irrep: int32 [64], replicated, may hold values from 0 to 7
- occ_energy: float32 [2048], P('occ'), may hold values from -1.5 to -0.5
- vir_energy: float32 [4096], P('vir'), may hold values from 0.5 to 2.5
Outputs:
- update: float32 [4096, 2048], P('vir', 'occ')
The draws below stay inside these ranges and needn't reach their ends.
All inputs are finite; a program needn't handle non-finite values.
Results may differ from the reference program's by a relative error of at most 0.0003.
Values may be sent and summed in bfloat16 or wider, within the bound.
A program may use at most 128 MiB of HBM per device.

```python
import jax
import jax.numpy as jnp

TILE = 64
P_SIZE = 2048
Q = 4096


def with_ends(array, own_key, low, top_value):
    spot = [jax.random.randint(jax.random.fold_in(own_key, axis), (), 0, length) for axis, length in enumerate(array.shape)]
    widest = array.shape.index(max(array.shape))
    neighbour = spot[:widest] + [(spot[widest] + 1) % array.shape[widest]] + spot[widest + 1:]
    return array.at[tuple(spot)].set(low).at[tuple(neighbour)].set(top_value)


def with_spikes(entries, key, source, target, blocks, factor):
    owner, partner = [(jnp.arange(entries.shape[position]) // (entries.shape[position] // blocks)).reshape([-1 if axis == position else 1 for axis in range(entries.ndim)]) for position in (source, target)]
    chosen = jax.random.permutation(key, blocks)[partner]
    strong = (owner == chosen) | (owner == (partner + blocks // 2) % blocks)
    return jnp.where(strong, factor * entries, entries)


def steps_of(stream_key, extent, shards, low, top_value):
    gain = 1.0
    for dim, blocks in shards:
        steps = jax.random.uniform(jax.random.fold_in(jax.random.fold_in(stream_key, 6), dim), (blocks,), jnp.float32, low / len(shards), top_value / len(shards))
        gain = gain * jnp.repeat(jnp.exp(steps), extent[dim] // blocks).reshape((-1,) + (1,) * (len(extent) - 1 - dim))
    return gain


def gaussian(stream_key, dims, width, limit, split=(), dtype=jnp.bfloat16):
    result = jax.random.normal(stream_key, dims, jnp.float32) * width
    if len(split) > 0:
        result = steps_of(stream_key, dims, split, -0.22, 0.18) * result
    return jnp.clip(result, min=-limit, max=limit).astype(dtype)


def heavy_noise(stream_key, shape, spread, most, pieces, heavy, dtype=jnp.bfloat16):
    result = spread * jax.random.normal(stream_key, shape, jnp.float32)
    if pieces:
        result = result * steps_of(stream_key, shape, pieces, -0.22, 0.18)
    return jnp.clip(with_spikes(result, jax.random.fold_in(stream_key, 3), *heavy), -most, most).astype(dtype)


def setup_inputs(seed: int = 0) -> dict:
    keys = jax.random.split(jax.random.key(seed), 8)
    amplitudes = gaussian(keys[0], (P_SIZE, Q), 1.0, 6.0, ((0, 4), (1, 8)))
    hole_integrals = gaussian(keys[1], (P_SIZE, P_SIZE), (P_SIZE // 8) ** -0.5, 0.375, ((0, 4),))
    particle_integrals = heavy_noise(keys[2], (Q, Q), (Q // 8) ** -0.5, 0.375, ((0, 8),), (0, 1, 8, 2.0))
    occ_irrep = with_ends(jax.random.randint(keys[3], (P_SIZE // TILE,), 0, 8), jax.random.fold_in(keys[3], 1), 0, 7).astype(jnp.int32)
    vir_irrep = with_ends(jax.random.randint(keys[4], (Q // TILE,), 0, 8), jax.random.fold_in(keys[4], 1), 0, 7).astype(jnp.int32)
    occ_energy = jnp.clip(-1.5 + 1.0 * jax.random.uniform(keys[5], (P_SIZE,), jnp.float32) ** steps_of(keys[5], (P_SIZE,), ((0, 4),), -0.2, 0.2), -1.5, -0.5)
    vir_energy = jnp.clip(0.5 + 2.0 * jax.random.uniform(keys[6], (Q,), jnp.float32) ** steps_of(keys[6], (Q,), ((0, 8),), -0.2, 0.2), 0.5, 2.5)
    return {"amplitudes": amplitudes, "hole_integrals": hole_integrals, "particle_integrals": particle_integrals, "occ_irrep": occ_irrep, "vir_irrep": vir_irrep, "occ_energy": occ_energy, "vir_energy": vir_energy}


def reference(amplitudes, hole_integrals, particle_integrals, occ_irrep, vir_irrep, occ_energy, vir_energy):
    occ_labels = jnp.repeat(occ_irrep, TILE)
    vir_labels = jnp.repeat(vir_irrep, TILE)
    zero_value = jnp.zeros((), jnp.bfloat16)
    hole_masked = jnp.where(occ_labels[:, None] == occ_labels[None, :], hole_integrals, zero_value)
    particle_masked = jnp.where(vir_labels[:, None] == vir_labels[None, :], particle_integrals, zero_value)
    hole = jnp.dot(hole_masked, amplitudes, preferred_element_type=jnp.float32)
    particle = jnp.dot(amplitudes, particle_masked, preferred_element_type=jnp.float32)
    energy_gap = vir_energy[:, None] - occ_energy[None, :]
    return (hole + particle).T / energy_gap
```

```python
import functools

import jax
import jax.numpy as jnp
from jax import lax
from jax.experimental import pallas as pl
from jax.experimental.pallas import tpu as pltpu
from jax.sharding import PartitionSpec as P

TILE = 64
CORES = 2
CHUNKS = 4
MESH = pl.DeviceIdType.MESH


def kernel(
    lines, width, groups, amp, hole, slab, occ_irrep, vir_irrep, occ_labels, vir_labels, occ_e, vir_e, out,
    slab_all, slab_masked, rows_all, cols_all, hole_masked, mine, theirs, acc,
    send_sem, slab_sem, rows_sem, cols_sem, part_sem, local_sem,
):
    p_own, q_own = amp.shape
    o, v = lax.axis_index("occ"), lax.axis_index("vir")
    h, c = o // CORES, lax.rem(o, CORES)
    z, x = v // width, lax.rem(v, width)
    occ_size = groups * CORES
    share = q_own // occ_size
    step_rows = p_own // CHUNKS
    partner = h * CORES + (1 - c)
    sent = []

    def shift(i, d, n):
        return lax.rem(i + d, n)

    others_h = [shift(h, d, groups) for d in range(1, groups)]
    others_z = [shift(z, d, lines) for d in range(1, lines)]
    others_x = [shift(x, d, width) for d in range(1, width)]

    def send(src, dst, recv, device, when=None):
        copy = pltpu.make_async_remote_copy(
            src_ref=src, dst_ref=dst, send_sem=send_sem.at[len(sent)], recv_sem=recv,
            device_id=device, device_id_type=MESH,
        )
        sent.append((copy, when))
        if when is None:
            copy.start()
        else:
            pl.when(when)(copy.start)

    def landed(ref, sem):
        pltpu.make_async_copy(ref, ref, sem).wait()

    barrier = pltpu.get_barrier_semaphore()
    peers = [(partner, v)] + [(g * CORES + c, v) for g in others_h]
    peers += [(o, g * width + x) for g in others_z] + [(o, z * width + g) for g in others_x]
    for peer in peers:
        pl.semaphore_signal(barrier, inc=1, device_id=peer, device_id_type=MESH)
    pl.semaphore_wait(barrier, len(peers))

    own_cols = pltpu.make_async_copy(
        slab.at[:, pl.ds(pl.multiple_of(z * width * q_own, q_own), width * q_own)],
        slab_all.at[pl.ds(pl.multiple_of(z * q_own, q_own), q_own), :],
        local_sem.at[0],
    )
    own_cols.start()
    own_rows = pltpu.make_async_copy(amp, rows_all.at[:, pl.ds(pl.multiple_of(z * q_own, q_own), q_own)], local_sem.at[1])
    own_rows.start()
    own_pairs = pltpu.make_async_copy(amp, cols_all.at[pl.ds(pl.multiple_of(o * p_own, p_own), p_own), :], local_sem.at[2])
    own_pairs.start()

    def slab_piece(zz, oo, xx):
        return slab_all.at[
            pl.ds(pl.multiple_of(zz * q_own + oo * share, share), share),
            pl.ds(pl.multiple_of(xx * q_own, q_own), q_own),
        ]

    def slab_send(xx):
        for zz in others_z:
            send(
                slab.at[
                    pl.ds(pl.multiple_of(o * share, share), share),
                    pl.ds(pl.multiple_of((zz * width + xx) * q_own, q_own), q_own),
                ],
                slab_piece(z, o, xx), slab_sem.at[z, o, xx], (o, zz * width + x),
            )

    def slab_share(xx):
        for zz in reversed(others_z):
            piece, sem = slab_piece(zz, o, xx), slab_sem.at[zz, o, xx]
            landed(piece, sem)
            for g in others_h:
                send(piece, piece, sem, (g * CORES + c, v))
            send(piece, piece, sem, (partner, v))

    def slab_pass(xx):
        for zz in reversed(others_z):
            for g in others_h:
                piece, sem = slab_piece(zz, g * CORES + c, xx), slab_sem.at[zz, g * CORES + c, xx]
                landed(piece, sem)
                send(piece, piece, sem, (partner, v))

    def slab_mask(xx):
        for zz in others_z:
            for g in range(groups):
                landed(slab_piece(zz, g * CORES + 1 - c, xx), slab_sem.at[zz, g * CORES + 1 - c, xx])
        tiles = q_own // TILE
        columns = pl.ds(pl.multiple_of(xx * q_own, q_own), q_own)
        labels = vir_labels[:, pl.ds(pl.multiple_of((z * width + xx) * q_own, q_own), q_own)]

        @pl.loop(0, lines * tiles)
        def _(i):
            label = vir_irrep[((i // tiles) * width + x) * tiles + lax.rem(i, tiles)]
            at = pl.ds(pl.multiple_of(i * TILE, TILE), TILE)
            block = slab_all[at, columns].astype(jnp.float32)
            slab_masked[at, columns] = jnp.where(labels == label, block, 0.0).astype(jnp.bfloat16)

    def rows_piece(zz, k):
        return rows_all.at[pl.ds(k * step_rows, step_rows), pl.ds(pl.multiple_of(zz * q_own, q_own), q_own)]

    up, down = (o, (z + 1) * width + x), (o, (z - 1) * width + x)
    has_up, has_down = z < lines - 1, z > 0

    def rows_send(k):
        src = amp.at[pl.ds(k * step_rows, step_rows), :]
        send(src, rows_piece(z, k), rows_sem.at[z, k], up, has_up)
        send(src, rows_piece(z, k), rows_sem.at[z, k], down, has_down)

    def rows_relay(k):
        for d in range(1, lines):
            for zz, there, onward, device in (
                (z - d, z - d >= 0, has_up, up), (z + d, z + d < lines, has_down, down),
            ):
                piece, sem = rows_piece(zz, k), rows_sem.at[lax.rem(zz + lines, lines), k]
                pl.when(there)(functools.partial(landed, piece, sem))
                if d < lines - 1:
                    send(piece, piece, sem, device, jnp.logical_and(there, onward))

    def pairs_piece(oo):
        return cols_all.at[pl.ds(pl.multiple_of(oo * p_own, p_own), p_own), :]

    for xx in others_x:
        slab_send(xx)
    for k in range(CHUNKS):
        rows_send(k)
    for g in others_h:
        send(amp, pairs_piece(o), cols_sem.at[o], (g * CORES + c, v))
    send(amp, pairs_piece(o), cols_sem.at[o], (partner, v))

    tiles = p_own // TILE

    @pl.loop(0, tiles)
    def _(i):
        at = pl.ds(pl.multiple_of(i * TILE, TILE), TILE)
        label = occ_irrep[o * tiles + i]
        hole_masked[at, :] = jnp.where(
            occ_labels[...] == label, hole[at, :].astype(jnp.float32), 0.0
        ).astype(jnp.bfloat16)

    for xx in others_x:
        slab_share(xx)
    rows_relay(0)
    for xx in others_x:
        slab_pass(xx)
    for k in range(1, CHUNKS):
        rows_relay(k)
    slab_send(x)
    for g in others_h:
        landed(pairs_piece(g * CORES + c), cols_sem.at[g * CORES + c])
        send(pairs_piece(g * CORES + c), pairs_piece(g * CORES + c), cols_sem.at[g * CORES + c], (partner, v))
    own_cols.wait()
    own_rows.wait()
    own_pairs.wait()
    for xx in others_x:
        slab_mask(xx)
        columns = pl.ds(pl.multiple_of(xx * q_own, q_own), q_own)
        slot = xx
        for k in range(CHUNKS):
            at = pl.ds(k * step_rows, step_rows)
            mine[slot, at, :] = jnp.dot(
                rows_all[at, :], slab_masked[:, columns], preferred_element_type=jnp.float32
            )
            send(
                mine.at[slot, at, :], theirs.at[x, at, :], part_sem.at[x, k], (o, z * width + xx)
            )
    slab_share(x)
    for g in range(groups):
        landed(pairs_piece(g * CORES + 1 - c), cols_sem.at[g * CORES + 1 - c])

    @pl.loop(0, CHUNKS)
    def _(k):
        at = pl.ds(pl.multiple_of(k * step_rows, step_rows), step_rows)
        acc[at, :] = jnp.dot(hole_masked[at, :], cols_all[...], preferred_element_type=jnp.float32)

    slab_pass(x)
    slab_mask(x)
    columns = pl.ds(pl.multiple_of(x * q_own, q_own), q_own)

    @pl.loop(0, CHUNKS)
    def _(k):
        at = pl.ds(pl.multiple_of(k * step_rows, step_rows), step_rows)
        acc[at, :] += jnp.dot(
            rows_all[at, :], slab_masked[:, columns], preferred_element_type=jnp.float32
        )

    for k in range(CHUNKS):
        at = pl.ds(k * step_rows, step_rows)
        total = acc[at, :]
        for xx in others_x:
            landed(theirs.at[xx, at, :], part_sem.at[xx, k])
            total = total + theirs[xx, at, :]
        out[:, at] = total.T / (vir_e[...] - occ_e[:, at])

    for copy, when in sent:
        if when is None:
            copy.wait_send()
        else:
            pl.when(when)(copy.wait_send)


def per_device(
    occ_size, vir_size, amplitudes, hole_integrals, particle_integrals, occ_irrep, vir_irrep, occ_energy, vir_energy
):
    width = 1
    while 4 * width * width <= vir_size:
        width *= 2
    lines, groups = vir_size // width, occ_size // CORES
    p_own, q_own = amplitudes.shape
    p_all = p_own * occ_size
    sends = (
        width * (lines - 1) * (2 * groups)
        + 2 * CHUNKS * (lines - 1)
        + 2 * groups - 1
        + (width - 1) * CHUNKS
    )
    vmem = pl.BlockSpec(memory_space=pltpu.VMEM)
    smem = pl.BlockSpec(memory_space=pltpu.SMEM)
    return pl.pallas_call(
        functools.partial(kernel, lines, width, groups),
        out_shape=jax.ShapeDtypeStruct((q_own, p_own), jnp.float32),
        in_specs=[vmem, vmem, pl.BlockSpec(memory_space=pl.ANY), smem, smem, vmem, vmem, vmem, vmem],
        out_specs=vmem,
        scratch_shapes=[
            pltpu.VMEM((lines * q_own, width * q_own), jnp.bfloat16),
            pltpu.VMEM((lines * q_own, width * q_own), jnp.bfloat16),
            pltpu.VMEM((p_own, lines * q_own), jnp.bfloat16),
            pltpu.VMEM((p_all, q_own), jnp.bfloat16),
            pltpu.VMEM((p_own, p_all), jnp.bfloat16),
            pltpu.VMEM((width, p_own, q_own), jnp.float32),
            pltpu.VMEM((width, p_own, q_own), jnp.float32),
            pltpu.VMEM((p_own, q_own), jnp.float32),
            pltpu.SemaphoreType.DMA((sends,)),
            pltpu.SemaphoreType.DMA((lines, occ_size, width)),
            pltpu.SemaphoreType.DMA((lines, CHUNKS)),
            pltpu.SemaphoreType.DMA((occ_size,)),
            pltpu.SemaphoreType.DMA((width, CHUNKS)),
            pltpu.SemaphoreType.DMA((3,)),
        ],
        compiler_params=pltpu.CompilerParams(
            collective_id=0, has_side_effects=True, vmem_limit_bytes=60 * 1024 * 1024
        ),
    )(
        amplitudes, hole_integrals, particle_integrals, occ_irrep, vir_irrep,
        jnp.repeat(occ_irrep, TILE)[None, :], jnp.repeat(vir_irrep, TILE)[None, :],
        occ_energy[None, :], vir_energy[:, None],
    )


def solution(mesh):
    placed = (P("occ", "vir"), P("occ", None), P("vir", None), P(), P(), P("occ"), P("vir"))
    return jax.shard_map(
        functools.partial(per_device, mesh.shape["occ"], mesh.shape["vir"]),
        mesh=mesh, in_specs=placed, out_specs=P("vir", "occ"), check_vma=False,
    )
```

```python
import functools

import jax
import jax.numpy as jnp
from jax import lax
from jax.experimental import pallas as pl
from jax.experimental.pallas import tpu as pltpu
from jax.sharding import PartitionSpec as P

TILE = 64
CORES = 2
CHUNKS = 4
MESH = pl.DeviceIdType.MESH


def kernel(
    lines, width, groups, amp, hole, slab, occ_irrep, vir_irrep, occ_e, vir_e, out,
    occ_labels, vir_labels,
    slab_all, slab_masked, rows_all, cols_all, hole_masked, mine, theirs, acc,
    send_sem, slab_sem, rows_sem, cols_sem, part_sem, local_sem,
):
    p_own, q_own = amp.shape
    o, v = lax.axis_index("occ"), lax.axis_index("vir")
    h, c = o // CORES, lax.rem(o, CORES)
    z, x = v // width, lax.rem(v, width)
    occ_size = groups * CORES
    share = q_own // occ_size
    step_rows = p_own // CHUNKS
    partner = h * CORES + (1 - c)
    sent = []

    def shift(i, d, n):
        return lax.rem(i + d, n)

    others_h = [shift(h, d, groups) for d in range(1, groups)]
    others_z = [shift(z, d, lines) for d in range(1, lines)]
    others_x = [shift(x, d, width) for d in range(1, width)]

    def send(src, dst, recv, device, when=None):
        copy = pltpu.make_async_remote_copy(
            src_ref=src, dst_ref=dst, send_sem=send_sem.at[len(sent)], recv_sem=recv,
            device_id=device, device_id_type=MESH,
        )
        sent.append((copy, when))
        if when is None:
            copy.start()
        else:
            pl.when(when)(copy.start)

    def landed(ref, sem):
        pltpu.make_async_copy(ref, ref, sem).wait()

    barrier = pltpu.get_barrier_semaphore()
    peers = [(partner, v)] + [(g * CORES + c, v) for g in others_h]
    peers += [(o, g * width + x) for g in others_z] + [(o, z * width + g) for g in others_x]
    for peer in peers:
        pl.semaphore_signal(barrier, inc=1, device_id=peer, device_id_type=MESH)
    pl.semaphore_wait(barrier, len(peers))

    own_cols = pltpu.make_async_copy(
        slab.at[:, pl.ds(pl.multiple_of(z * width * q_own, q_own), width * q_own)],
        slab_all.at[pl.ds(pl.multiple_of(z * q_own, q_own), q_own), :],
        local_sem.at[0],
    )
    own_cols.start()
    own_rows = pltpu.make_async_copy(amp, rows_all.at[:, pl.ds(pl.multiple_of(z * q_own, q_own), q_own)], local_sem.at[1])
    own_rows.start()
    own_pairs = pltpu.make_async_copy(amp, cols_all.at[pl.ds(pl.multiple_of(o * p_own, p_own), p_own), :], local_sem.at[2])
    own_pairs.start()

    def slab_piece(zz, oo, xx):
        return slab_all.at[
            pl.ds(pl.multiple_of(zz * q_own + oo * share, share), share),
            pl.ds(pl.multiple_of(xx * q_own, q_own), q_own),
        ]

    def slab_send(xx):
        for zz in others_z:
            send(
                slab.at[
                    pl.ds(pl.multiple_of(o * share, share), share),
                    pl.ds(pl.multiple_of((zz * width + xx) * q_own, q_own), q_own),
                ],
                slab_piece(z, o, xx), slab_sem.at[z, o, xx], (o, zz * width + x),
            )

    def slab_share(xx):
        for zz in reversed(others_z):
            piece, sem = slab_piece(zz, o, xx), slab_sem.at[zz, o, xx]
            landed(piece, sem)
            for g in others_h:
                send(piece, piece, sem, (g * CORES + c, v))
            send(piece, piece, sem, (partner, v))

    def slab_pass(xx):
        for zz in reversed(others_z):
            for g in others_h:
                piece, sem = slab_piece(zz, g * CORES + c, xx), slab_sem.at[zz, g * CORES + c, xx]
                landed(piece, sem)
                send(piece, piece, sem, (partner, v))

    def slab_mask(xx):
        for zz in others_z:
            for g in range(groups):
                landed(slab_piece(zz, g * CORES + 1 - c, xx), slab_sem.at[zz, g * CORES + 1 - c, xx])
        tiles = q_own // TILE
        columns = pl.ds(pl.multiple_of(xx * q_own, q_own), q_own)
        labels = vir_labels[:, pl.ds(pl.multiple_of((z * width + xx) * q_own, q_own), q_own)]

        @pl.loop(0, lines * tiles)
        def _(i):
            label = vir_irrep[((i // tiles) * width + x) * tiles + lax.rem(i, tiles)]
            at = pl.ds(pl.multiple_of(i * TILE, TILE), TILE)
            block = slab_all[at, columns].astype(jnp.float32)
            slab_masked[at, columns] = jnp.where(labels == label, block, 0.0).astype(jnp.bfloat16)

    def rows_piece(zz, k):
        return rows_all.at[pl.ds(k * step_rows, step_rows), pl.ds(pl.multiple_of(zz * q_own, q_own), q_own)]

    up, down = (o, (z + 1) * width + x), (o, (z - 1) * width + x)
    has_up, has_down = z < lines - 1, z > 0

    def rows_send(k):
        src = amp.at[pl.ds(k * step_rows, step_rows), :]
        send(src, rows_piece(z, k), rows_sem.at[z, k], up, has_up)
        send(src, rows_piece(z, k), rows_sem.at[z, k], down, has_down)

    def rows_relay(k, distances):
        for d in distances:
            for zz, there, onward, device in (
                (z - d, z - d >= 0, has_up, up), (z + d, z + d < lines, has_down, down),
            ):
                piece, sem = rows_piece(zz, k), rows_sem.at[lax.rem(zz + lines, lines), k]
                pl.when(there)(functools.partial(landed, piece, sem))
                if d < lines - 1:
                    send(piece, piece, sem, device, jnp.logical_and(there, onward))

    def pairs_piece(oo):
        return cols_all.at[pl.ds(pl.multiple_of(oo * p_own, p_own), p_own), :]

    for xx in others_x:
        slab_send(xx)
    for k in range(CHUNKS):
        rows_send(k)
    for g in others_h:
        send(amp, pairs_piece(o), cols_sem.at[o], (g * CORES + c, v))
    send(amp, pairs_piece(o), cols_sem.at[o], (partner, v))

    tiles = p_own // TILE

    half = lax.broadcasted_iota(jnp.int32, (1, 2 * TILE), 1) < TILE
    for labels, irreps in ((occ_labels, occ_irrep), (vir_labels, vir_irrep)):

        @pl.loop(0, irreps.shape[0] // 2)
        def _(i):
            labels[:, pl.ds(pl.multiple_of(i * 2 * TILE, 2 * TILE), 2 * TILE)] = jnp.where(
                half, irreps[2 * i], irreps[2 * i + 1]
            )

    @pl.loop(0, tiles)
    def _(i):
        at = pl.ds(pl.multiple_of(i * TILE, TILE), TILE)
        label = occ_irrep[o * tiles + i]
        hole_masked[at, :] = jnp.where(
            occ_labels[...] == label, hole[at, :].astype(jnp.float32), 0.0
        ).astype(jnp.bfloat16)

    for xx in others_x:
        slab_share(xx)
    for k in range(CHUNKS):
        rows_relay(k, range(1, 2))
    slab_send(x)
    for xx in others_x:
        slab_pass(xx)
    for g in others_h:
        landed(pairs_piece(g * CORES + c), cols_sem.at[g * CORES + c])
        send(pairs_piece(g * CORES + c), pairs_piece(g * CORES + c), cols_sem.at[g * CORES + c], (partner, v))
    own_cols.wait()
    own_rows.wait()
    own_pairs.wait()
    for xx in others_x:
        slab_mask(xx)
    for k in range(CHUNKS):
        rows_relay(k, range(2, lines))
        at = pl.ds(k * step_rows, step_rows)
        for xx in others_x:
            columns = pl.ds(pl.multiple_of(xx * q_own, q_own), q_own)
            mine[xx, at, :] = jnp.dot(
                rows_all[at, :], slab_masked[:, columns], preferred_element_type=jnp.float32
            )
            send(
                mine.at[xx, at, :], theirs.at[x, at, :], part_sem.at[x, k], (o, z * width + xx)
            )
    slab_share(x)
    for g in range(groups):
        landed(pairs_piece(g * CORES + 1 - c), cols_sem.at[g * CORES + 1 - c])

    @pl.loop(0, CHUNKS)
    def _(k):
        at = pl.ds(pl.multiple_of(k * step_rows, step_rows), step_rows)
        acc[at, :] = jnp.dot(hole_masked[at, :], cols_all[...], preferred_element_type=jnp.float32)

    slab_pass(x)
    slab_mask(x)
    columns = pl.ds(pl.multiple_of(x * q_own, q_own), q_own)

    @pl.loop(0, CHUNKS)
    def _(k):
        at = pl.ds(pl.multiple_of(k * step_rows, step_rows), step_rows)
        acc[at, :] += jnp.dot(
            rows_all[at, :], slab_masked[:, columns], preferred_element_type=jnp.float32
        )

    vir_column = jnp.broadcast_to(vir_e[...], (step_rows, q_own)).T
    for k in range(CHUNKS):
        at = pl.ds(k * step_rows, step_rows)
        total = acc[at, :]
        for xx in others_x:
            landed(theirs.at[xx, at, :], part_sem.at[xx, k])
            total = total + theirs[xx, at, :]
        out[:, at] = total.T / (vir_column - occ_e[:, at])

    for copy, when in sent:
        if when is None:
            copy.wait_send()
        else:
            pl.when(when)(copy.wait_send)


def per_device(
    occ_size, vir_size, amplitudes, hole_integrals, particle_integrals, occ_irrep, vir_irrep, occ_energy, vir_energy
):
    width = 1
    while 4 * width * width <= vir_size:
        width *= 2
    lines, groups = vir_size // width, occ_size // CORES
    p_own, q_own = amplitudes.shape
    p_all = p_own * occ_size
    sends = (
        width * (lines - 1) * (2 * groups)
        + 2 * CHUNKS * (lines - 1)
        + 2 * groups - 1
        + (width - 1) * CHUNKS
    )
    vmem = pl.BlockSpec(memory_space=pltpu.VMEM)
    smem = pl.BlockSpec(memory_space=pltpu.SMEM)
    return pl.pallas_call(
        functools.partial(kernel, lines, width, groups),
        out_shape=jax.ShapeDtypeStruct((q_own, p_own), jnp.float32),
        in_specs=[vmem, vmem, pl.BlockSpec(memory_space=pl.ANY), smem, smem, vmem, vmem],
        out_specs=vmem,
        scratch_shapes=[
            pltpu.VMEM((1, occ_irrep.shape[0] * TILE), jnp.int32),
            pltpu.VMEM((1, vir_irrep.shape[0] * TILE), jnp.int32),
            pltpu.VMEM((lines * q_own, width * q_own), jnp.bfloat16),
            pltpu.VMEM((lines * q_own, width * q_own), jnp.bfloat16),
            pltpu.VMEM((p_own, lines * q_own), jnp.bfloat16),
            pltpu.VMEM((p_all, q_own), jnp.bfloat16),
            pltpu.VMEM((p_own, p_all), jnp.bfloat16),
            pltpu.VMEM((width, p_own, q_own), jnp.float32),
            pltpu.VMEM((width, p_own, q_own), jnp.float32),
            pltpu.VMEM((p_own, q_own), jnp.float32),
            pltpu.SemaphoreType.DMA((sends,)),
            pltpu.SemaphoreType.DMA((lines, occ_size, width)),
            pltpu.SemaphoreType.DMA((lines, CHUNKS)),
            pltpu.SemaphoreType.DMA((occ_size,)),
            pltpu.SemaphoreType.DMA((width, CHUNKS)),
            pltpu.SemaphoreType.DMA((3,)),
        ],
        compiler_params=pltpu.CompilerParams(
            collective_id=0, has_side_effects=True, vmem_limit_bytes=60 * 1024 * 1024
        ),
    )(
        amplitudes, hole_integrals, particle_integrals, occ_irrep, vir_irrep,
        occ_energy[None, :], vir_energy[None, :],
    )


def solution(mesh):
    placed = (P("occ", "vir"), P("occ", None), P("vir", None), P(), P(), P("occ"), P("vir"))
    return jax.shard_map(
        functools.partial(per_device, mesh.shape["occ"], mesh.shape["vir"]),
        mesh=mesh, in_specs=placed, out_specs=P("vir", "occ"), check_vma=False,
    )
```
